8 devices in a mesh: fld: 1 (over z), col: 2 (over y), row: 4 (over x, core).
Axes of the slice: x: 2, y: 2, z: 1, core: 2. Of those that a mesh axis runs over, the one named last changes fastest.
Arguments:
- u_real: float32 [6, 240, 240, 240], P('fld', None, 'row', 'col')
- u_imag: float32 [6, 240, 240, 240], P('fld', None, 'row', 'col')
- g_filter: float32 [240, 240, 240], P('row', 'col')
Outputs:
- output 1: float32 [6, 240, 240, 240], P('fld', 'row', 'col')
- output 2: float32 [6, 240, 240, 240], P('fld', 'row', 'col')
All inputs are finite; a program needn't handle non-finite values.
Results may differ from the reference program's by a relative error of at most 0.001.
Values are sent between devices in bfloat16 or wider.
A program may use at most 1 GiB of HBM per device.

```python
import jax
import jax.numpy as jnp
from jax import lax

N = 240
BATCH = 6


def setup_inputs(seed: int = 0, part: int = 0) -> dict:
    root_key = jax.random.key(seed)
    field_key = jax.random.fold_in(jax.random.fold_in(root_key, 1), part)
    key_re, key_im = jax.random.split(field_key)
    u_real = jax.random.normal(key_re, (BATCH, N, N, N), jnp.float32)
    u_imag = jax.random.normal(key_im, (BATCH, N, N, N), jnp.float32)
    wave_num = ((jnp.arange(N) + N // 2) % N - N // 2).astype(jnp.float32)
    wave_sq = wave_num * wave_num
    k_sq = wave_sq[:, None, None] + wave_sq[None, :, None] + wave_sq[None, None, :]
    profile = 2.0 / (1.0 + 16.0 * k_sq / (N * N))
    jitter = jax.random.uniform(jax.random.fold_in(root_key, 2), (N, N, N), jnp.float32)
    g_filter = profile * (0.5 + jitter)
    return {"u_real": u_real, "u_imag": u_imag, "g_filter": g_filter}


def reference(u_real, u_imag, g_filter):
    def one_field(field_pair):
        field_re, field_im = field_pair
        spectrum = jnp.fft.fftn(field_re + 1j * field_im, norm="ortho")
        filtered = spectrum * g_filter
        return jnp.real(filtered).astype(jnp.float32), jnp.imag(filtered).astype(jnp.float32)
    w_real, w_imag = lax.map(one_field, (u_real, u_imag))
    return w_real, w_imag
```

```python
import math
import numpy as np
import jax
import jax.numpy as jnp
from jax import lax
from jax.experimental import pallas as pl
from jax.experimental.pallas import tpu as pltpu
from jax.sharding import PartitionSpec as P

N = 240
PARTS = 2
HIGHEST = lax.Precision.HIGHEST


def dft_parts():
    k = np.arange(N)
    angle = 2.0 * math.pi * ((k[:, None] * k[None, :]) % N) / N
    return np.cos(angle) / math.sqrt(N), np.sin(angle) / math.sqrt(N)


def dft_x():
    cos, sin = dft_parts()
    mat = np.zeros((N, 2, 2, N))
    mat[:, 0, 0], mat[:, 0, 1] = cos, sin
    mat[:, 1, 0], mat[:, 1, 1] = -sin, cos
    return mat.reshape(2 * N, 2 * N).astype(np.float32)


def dft_y(rows, cols):
    cos, sin = dft_parts()
    mat = np.zeros((2, N, 2, N))
    mat[0, :, 0], mat[0, :, 1] = cos, sin
    mat[1, :, 0], mat[1, :, 1] = -sin, cos
    mat = mat.reshape(2, cols, N // cols, 2, rows, N // rows)
    return mat.transpose(1, 0, 2, 4, 3, 5).reshape(2 * N, 2 * N).astype(np.float32)


def dft_z(cols):
    cos, sin = dft_parts()
    half = N // cols
    mat = np.zeros((cols, 2, 128, 2, 256))
    for b in range(cols):
        part = slice(b * half, (b + 1) * half)
        mat[b, 0, :half, 0, :N], mat[b, 1, :half, 0, :N] = cos[part], sin[part]
        mat[b, 0, :half, 1, :N], mat[b, 1, :half, 1, :N] = -sin[part], cos[part]
    return mat.reshape(cols * 256, 512).astype(np.float32)


def pad_lanes(v):
    return jnp.concatenate([v, jnp.zeros(v.shape[:-1] + (8,), v.dtype)], axis=-1)


def x_body(yb, ur, ui, mat, *outs):
    def pair(p, carry):
        y = 2 * p
        re = jnp.concatenate([pad_lanes(ur[0, y]), pad_lanes(ur[0, y + 1])], axis=1)
        im = jnp.concatenate([pad_lanes(ui[0, y]), pad_lanes(ui[0, y + 1])], axis=1)
        res = jnp.dot(mat[...], jnp.concatenate([re, im], axis=0), precision=HIGHEST, preferred_element_type=jnp.float32)
        row = pl.program_id(0) * yb + y
        for d, out in enumerate(outs):
            size = 480 // len(outs)
            out[pl.ds(row, size, stride=60), :] = res[d * size:(d + 1) * size, :128]
            out[pl.ds(row + 1, size, stride=60), :] = res[d * size:(d + 1) * size, 128:]
        return carry
    lax.fori_loop(0, yb // 2, pair, 0)


def y_body(kb, r0, r1, r2, r3, mat, t0, t1):
    def pair(p, carry):
        k = 2 * p
        def column(kx):
            return jnp.concatenate([r[kx] for r in (r0, r1, r2, r3)], axis=0)
        rhs = jnp.concatenate([column(k), column(k + 1)], axis=1)
        res = jnp.dot(mat[...], rhs, precision=HIGHEST, preferred_element_type=jnp.float32)
        for j in range(2):
            t0[k + j] = res[:240, j * 128:(j + 1) * 128]
            t1[k + j] = res[240:, j * 128:(j + 1) * 128]
        return carry
    lax.fori_loop(0, kb // 2, pair, 0)


def z_body(kb, q0, q1, g, mat, *refs):
    wr, wi = refs[-2:]
    def pair(p, carry):
        k = 2 * p
        def line(kx):
            return jnp.concatenate([q[kx, c * 120:(c + 1) * 120] for q in (q0, q1) for c in range(2)], axis=1)
        lhs = jnp.concatenate([line(k), line(k + 1)], axis=0)
        res = jnp.dot(lhs, mat[...], precision=HIGHEST, preferred_element_type=jnp.float32)
        for j in range(2):
            part = res[j * 120:(j + 1) * 120]
            wr[0, k + j] = part[:, :240] * g[k + j]
            wi[0, k + j] = part[:, 256:496] * g[k + j]
        return carry
    lax.fori_loop(0, kb // 2, pair, 0)


def solution(mesh):
    rows, cols = mesh.shape["row"], mesh.shape["col"]
    params = pltpu.CompilerParams(vmem_limit_bytes=56 * 2**20)
    cost = pl.CostEstimate(flops=6 * 2 * 480 * 480 * 7200, bytes_accessed=30_000_000, transcendentals=0)
    f32 = jnp.float32

    def local_forward(u_real, u_imag, g_filter):
        fields = u_real.shape[0]
        ur = jnp.transpose(u_real, (0, 2, 1, 3))
        ui = jnp.transpose(u_imag, (0, 2, 1, 3))
        me_row, me_col = lax.axis_index("row"), lax.axis_index("col")
        mat_x = jnp.asarray(dft_x()).reshape(4, 120, 480)
        mat_x = jnp.concatenate([mat_x[me_row ^ d] for d in range(4)], axis=0)
        parts, lines = PARTS, 60 // PARTS
        mat_y = jnp.asarray(dft_y(rows, cols)).reshape(2, 240, 4, 120)
        mat_y = jnp.concatenate([mat_y[me_col ^ d] for d in range(2)], axis=0)
        mat_y = jnp.concatenate([mat_y[:, me_row ^ d] for d in range(4)], axis=1)
        mat_z = jnp.asarray(dft_z(cols)).reshape(2, 256, 512)
        mat_z = jnp.concatenate([mat_z[me_col ^ d] for d in range(2)], axis=0)
        full = pl.BlockSpec((480, 480), lambda i: (0, 0), pipeline_mode=pl.Buffered(1))
        yb, kb, zb = 12, 10, 6

        def x_step(f):
            spec = pl.BlockSpec((1, yb, N, 120), lambda i: (f, i, 0, 0))
            out = pl.BlockSpec((lines * 120, 128), lambda i: (0, 0), pipeline_mode=pl.Buffered(1))
            return pl.pallas_call(
                lambda *a: x_body(yb, *a), grid=(60 // yb,), in_specs=[spec, spec, full],
                out_specs=[out] * (4 * parts), out_shape=[jax.ShapeDtypeStruct((lines * 120, 128), f32)] * (4 * parts),
                compiler_params=params, cost_estimate=cost, name="xstep")(ur, ui, mat_x)

        def y_step(r):
            spec = pl.BlockSpec((kb, 120, 128), lambda i: (i, 0, 0))
            out = pl.BlockSpec((kb, 240, 128), lambda i: (i, 0, 0))
            return pl.pallas_call(
                lambda *a: y_body(kb, *a), grid=(lines // kb,), in_specs=[spec] * 4 + [full],
                out_specs=[out] * 2, out_shape=[jax.ShapeDtypeStruct((lines, 240, 128), f32)] * 2,
                compiler_params=params, cost_estimate=cost, name="ystep")(*r, mat_y)

        def z_step(f, h, q, w):
            spec = pl.BlockSpec((1, zb, 120, N), lambda i: (f, h * (lines // zb) + i, 0, 0))
            shape = jax.ShapeDtypeStruct((fields, 60, 120, N), f32)
            extra = [] if w is None else list(w)
            qs = pl.BlockSpec((zb, 240, 128), lambda i: (i, 0, 0))
            return pl.pallas_call(
                lambda *a: z_body(zb, *a), grid=(lines // zb,),
                in_specs=[qs, qs, pl.BlockSpec((zb, 120, N), lambda i: (h * (lines // zb) + i, 0, 0)),
                          pl.BlockSpec((512, 512), lambda i: (0, 0), pipeline_mode=pl.Buffered(1))] + [pl.BlockSpec(memory_space=pl.ANY)] * len(extra),
                out_specs=[spec, spec], out_shape=[shape, shape],
                input_output_aliases={4: 0, 5: 1} if extra else {},
                compiler_params=params, cost_estimate=cost, name="zstep")(*q, g_filter, mat_z, *extra)

        w, pending, step = None, [], 0
        for f in range(fields):
            s = [v.reshape(lines, 120, 128) for v in x_step(f)]
            for h in range(parts):
                r = [s[h]] + [lax.ppermute(s[d * parts + h], "row", [(i, i ^ d) for i in range(rows)]) for d in range(1, 4)]
                if len(pending) == 2:
                    w = z_step(*pending.pop(0), w)
                    r, w = lax.optimization_barrier((r, w))
                t = y_step(r)
                q = [t[0], lax.ppermute(t[1], "col", [(i, i ^ 1) for i in range(cols)])]
                pending.append((f, h, q))
        for item in pending:
            w = z_step(*item, w)
        return w[0], w[1]

    field_spec = P("fld", None, "row", "col")
    out_spec = P("fld", "row", "col", None)
    return jax.shard_map(local_forward, mesh=mesh, in_specs=(field_spec, field_spec, P("row", "col", None)), out_specs=(out_spec, out_spec), check_vma=False)
```

```python
import math
import numpy as np
import jax
import jax.numpy as jnp
from jax import lax
from jax.experimental import pallas as pl
from jax.experimental.pallas import tpu as pltpu
from jax.sharding import PartitionSpec as P

N = 240
HALF = N // 2
LANES = 128
SLOTS = 57
SPARE = LANES - HALF
SPREAD = HALF // SPARE
PARTS = 3
LINES = 60 // PARTS
ROWS = 2 * LINES
PITCH = 248
HIGHEST = lax.Precision.HIGHEST
f32 = jnp.float32


def dot(a, b):
    return jnp.dot(a, b, precision=HIGHEST, preferred_element_type=f32)


def half_matrices():
    k, n = np.arange(HALF), np.arange(HALF)
    mats = []
    for odd in range(2):
        angle = 2.0 * math.pi * ((k[:, None] * (2 * n + odd)[None, :]) % N) / N
        cos, sin = np.cos(angle) / math.sqrt(N), np.sin(angle) / math.sqrt(N)
        mats.append(np.stack([np.stack([cos, sin], axis=1), np.stack([-sin, cos], axis=1)]))
    return np.stack(mats)


def x_matrices():
    mat = half_matrices().reshape(2, 2, 2, PARTS, LINES, 2, HALF)
    return mat.transpose(2, 0, 3, 4, 1, 5, 6).reshape(2, 2, PARTS, ROWS, N).astype(np.float32)


def y_matrices(rows):
    mat = half_matrices().reshape(2, N, 2, rows, HALF // rows)
    return mat.transpose(0, 3, 1, 2, 4).astype(np.float32)


def z_matrix(cols):
    k = np.arange(N)
    angle = 2.0 * math.pi * ((k[:, None] * k[None, :]) % N) / N
    cos, sin = np.cos(angle) / math.sqrt(N), np.sin(angle) / math.sqrt(N)
    mat = np.zeros((cols, 2, LANES, 2, 256))
    for b in range(cols):
        part = slice(b * HALF, (b + 1) * HALF)
        mat[b, 0, :HALF, 0, :N], mat[b, 1, :HALF, 0, :N] = cos[part], sin[part]
        mat[b, 0, :HALF, 1, :N], mat[b, 1, :HALF, 1, :N] = -sin[part], cos[part]
    return mat.reshape(cols, 2 * LANES, 512).astype(np.float32)


def lane_index(rows):
    return lax.broadcasted_iota(jnp.int32, (rows, LANES), 1)


def gather_spread(parts):
    lane = lane_index(8)
    out = jnp.zeros((8, LANES), f32)
    for m, part in enumerate(parts):
        moved = pltpu.roll(part, (SPARE * m - HALF) % LANES, 1)
        out = jnp.where((lane >= SPARE * m) & (lane < SPARE * (m + 1)), moved, out)
    return out


def x_body(parts, ur, ui, er, ei, mat_e, mat_o, *refs):
    outs = refs[-4 * parts:]
    block = SLOTS // 3
    lane = lane_index(HALF)

    def samples(slot, odd):
        j = pl.program_id(0) * block + slot
        shift = HALF - SPARE * lax.rem(j, SPREAD)
        extra = jnp.minimum(j // SPREAD, 2)
        own = pl.ds(odd, HALF, stride=2)
        pieces = []
        for u, e in ((ur, er), (ui, ei)):
            moved = pltpu.roll(e.at[0, extra][own, :], shift, 1)
            pieces.append(jnp.where(lane < HALF, u.at[0, slot][own, :], moved))
        return jnp.concatenate(pieces, axis=0)

    def transform(slots):
        even = dot(mat_e[...], jnp.concatenate([samples(s, 0) for s in slots], axis=1))
        odd = dot(mat_o[...], jnp.concatenate([samples(s, 1) for s in slots], axis=1))
        both = (even + odd, even - odd)
        for i, s in enumerate(slots):
            for p in range(parts):
                for d in range(4):
                    row = (p * 2 + d % 2) * ROWS
                    outs[4 * p + d][s] = both[d // 2][row:row + ROWS, i * LANES:(i + 1) * LANES]

    def pair(p, carry):
        transform([2 * p, 2 * p + 1])
        return carry

    lax.fori_loop(0, block // 2, pair, 0)
    transform([block - 1])


def y_body(r0, r1, r2, r3, mat_e, mat_o, *refs):
    own, other, lines = refs[-3:]
    for d, r in enumerate((r0, r1, r2, r3)):
        groups = [r[j] for j in range(SLOTS)]
        groups += [gather_spread(groups[SPREAD * i:SPREAD * (i + 1)]) for i in range(3)]
        for y, v in enumerate(groups):
            lines[pl.ds(y % 2 * HALF + d * 30 + y // 2, 8, stride=PITCH), :] = v
    lane = lane_index(8)
    for p in range(2):
        def samples(odd):
            columns = []
            for kx in (2 * p, 2 * p + 1):
                columns.append(jnp.concatenate([lines[(2 * kx + c) * PITCH + odd * HALF:][:HALF] if False else lines[pl.ds((2 * kx + c) * PITCH + odd * HALF, HALF), :] for c in range(2)], axis=0))
            return jnp.concatenate(columns, axis=1)
        even = dot(mat_e[...], samples(0))
        odd = dot(mat_o[...], samples(1))
        mine, sent = even + odd, even - odd
        own[2 * p] = mine[:, :LANES]
        own[2 * p + 1] = mine[:, LANES:]
        groups = [sent[8 * (j % 30):8 * (j % 30) + 8, j // 30 * LANES:(j // 30 + 1) * LANES] for j in range(60)]
        for j in range(SLOTS):
            v = groups[j]
            if j < 3 * SPREAD:
                v = jnp.where(lane < HALF, v, pltpu.roll(groups[SLOTS + j // SPREAD], HALF - SPARE * (j % SPREAD), 1))
            other[p, 8 * j:8 * j + 8] = v


def z_body(kb, t, q, g, mat, *refs):
    wr, wi, line = refs[-3:]
    lane = lane_index(N)

    def pair(p, carry):
        for j in range(2):
            line[2 * j] = jnp.where(lane < HALF, t[2 * p + j], 0.0)
        line[1] = jnp.where(lane < HALF, q[p, :N], 0.0)
        line[3, :216] = jnp.where(lane[:216] < HALF, q[p, N:], 0.0)
        for i in range(3):
            line[3, 216 + 8 * i:224 + 8 * i] = gather_spread([q[p, 8 * j:8 * j + 8] for j in range(SPREAD * i, SPREAD * (i + 1))])
        lhs = jnp.concatenate([jnp.concatenate([line[2 * j + b, c * HALF:(c + 1) * HALF] for b in range(2) for c in range(2)], axis=1)
                               for j in range(2)], axis=0)
        res = dot(lhs, mat[...])
        for j in range(2):
            part = res[j * HALF:(j + 1) * HALF]
            wr[0, 2 * p + j] = part[:, :N] * g[2 * p + j]
            wi[0, 2 * p + j] = part[:, 256:256 + N] * g[2 * p + j]
        return carry

    lax.fori_loop(0, kb // 2, pair, 0)


def solution(mesh):
    rows, cols = mesh.shape["row"], mesh.shape["col"]
    params = pltpu.CompilerParams(vmem_limit_bytes=63 * 2**20)
    cost = pl.CostEstimate(flops=6 * 2 * 480 * 480 * 7200, bytes_accessed=30_000_000, transcendentals=0)
    once = pl.Buffered(1)
    unread = pl.BlockSpec(memory_space=pl.ANY)

    def local_forward(u_real, u_imag, g_filter):
        fields = u_real.shape[0]
        ur, ui = jnp.transpose(u_real, (0, 2, 1, 3)), jnp.transpose(u_imag, (0, 2, 1, 3))
        me_row, me_col = lax.axis_index("row"), lax.axis_index("col")
        core, chip = me_row % 2, me_row // 2
        mat_x = jnp.asarray(x_matrices())
        mat_x = jnp.stack([mat_x[core], mat_x[1 - core]], axis=2)
        sign_x = jnp.where(chip == 0, 1.0, -1.0).astype(f32)
        xe, xo = mat_x[0].reshape(N, N), sign_x * mat_x[1].reshape(N, N)
        mat_y = jnp.asarray(y_matrices(rows))
        mat_y = jnp.stack([mat_y[:, me_row ^ d] for d in range(rows)], axis=3)
        sign_y = jnp.where(me_col == 0, 1.0, -1.0).astype(f32)
        ye, yo = mat_y[0].reshape(N, N), sign_y * mat_y[1].reshape(N, N)
        mat_z = jnp.asarray(z_matrix(cols))
        mat_z = jnp.concatenate([mat_z[me_col ^ d] for d in range(cols)], axis=0)
        last = []

        def call(body, args, specs, **kw):
            out = pl.pallas_call(body, in_specs=specs + [unread] * len(last), compiler_params=params, cost_estimate=cost, **kw)(*args, *last)
            last[:] = [out[0]]
            return out

        def x_step(f, first, parts):
            block = SLOTS // 3
            spec = pl.BlockSpec((1, block, N, LANES), lambda i: (f, i, 0, 0))
            extra = pl.BlockSpec((1, 3, N, LANES), lambda i: (f, SLOTS // 3, 0, 0), pipeline_mode=once)
            mat = pl.BlockSpec((parts * 2 * ROWS, N), lambda i: (first // parts, 0), pipeline_mode=once)
            return call(
                lambda *a: x_body(parts, *a), (ur, ui, ur, ui, xe, xo), [spec, spec, extra, extra, mat, mat], grid=(3,),
                out_specs=[pl.BlockSpec((block, ROWS, LANES), lambda i: (i, 0, 0))] * (4 * parts),
                out_shape=[jax.ShapeDtypeStruct((SLOTS, ROWS, LANES), f32)] * (4 * parts), name="xstep")

        def y_step(r):
            mat = pl.BlockSpec((N, N), lambda i: (0, 0), pipeline_mode=once)
            return call(
                y_body, (*r, ye, yo), [pl.BlockSpec((SLOTS, 8, LANES), lambda i: (0, i, 0))] * 4 + [mat, mat], grid=(LINES // 4,),
                out_specs=[pl.BlockSpec((4, N, LANES), lambda i: (i, 0, 0)), pl.BlockSpec((2, 8 * SLOTS, LANES), lambda i: (i, 0, 0))],
                out_shape=[jax.ShapeDtypeStruct((LINES, N, LANES), f32), jax.ShapeDtypeStruct((LINES // 2, 8 * SLOTS, LANES), f32)],
                scratch_shapes=[pltpu.VMEM((8 * PITCH, LANES), f32)], name="ystep")

        def z_step(f, h, t, q, w):
            kb = 4
            lines = lambda i: h * (LINES // kb) + i
            spec = pl.BlockSpec((1, kb, HALF, N), lambda i: (f, lines(i), 0, 0))
            shape = jax.ShapeDtypeStruct((fields, 60, HALF, N), f32)
            return call(
                lambda *a: z_body(kb, *a), (t, q, g_filter, mat_z, *w),
                [pl.BlockSpec((kb, N, LANES), lambda i: (i, 0, 0)), pl.BlockSpec((kb // 2, 8 * SLOTS, LANES), lambda i: (i, 0, 0)),
                 pl.BlockSpec((kb, HALF, N), lambda i: (lines(i), 0, 0)), pl.BlockSpec((512, 512), lambda i: (0, 0), pipeline_mode=once)]
                + [unread] * len(w),
                grid=(LINES // kb,), out_specs=[spec, spec], out_shape=[shape, shape], input_output_aliases={4: 0, 5: 1} if w else {},
                scratch_shapes=[pltpu.VMEM((4, N, LANES), f32)], name="zstep")

        arrived = {}

        def send_x(f, first, parts):
            s = x_step(f, first, parts)
            for p in range(parts):
                mine = s[4 * p:4 * p + 4]
                arrived[f * PARTS + first + p] = [mine[0]] + [lax.ppermute(mine[d], "row", [(i, i ^ d) for i in range(rows)]) for d in range(1, 4)]

        for p in range(PARTS):
            send_x(0, p, 1)
        send_x(1, 0, PARTS)
        w, waiting = (), None
        for k in range(fields * PARTS):
            t, sent = y_step(arrived.pop(k))
            q = lax.ppermute(sent, "col", [(i, i ^ 1) for i in range(cols)])
            if k % PARTS == 0 and k // PARTS + 2 < fields:
                send_x(k // PARTS + 2, 0, PARTS)
            if waiting:
                w = z_step(*waiting, w)
            waiting = (k // PARTS, k % PARTS, t, q)
        w = z_step(*waiting, w)
        return w[0], w[1]

    field_spec = P("fld", None, "row", "col")
    out_spec = P("fld", "row", "col", None)
    return jax.shard_map(local_forward, mesh=mesh, in_specs=(field_spec, field_spec, P("row", "col", None)), out_specs=(out_spec, out_spec), check_vma=False)
```

```python
import math
import numpy as np
import jax
import jax.numpy as jnp
from jax import lax
from jax.experimental import pallas as pl
from jax.experimental.pallas import tpu as pltpu
from jax.sharding import PartitionSpec as P


N = 240
HALF = N // 2
LANES = 128
SLOTS = 57
SPARE = LANES - HALF
SPREAD = HALF // SPARE
PARTS = 3
X_BLOCK = 4
Y_UNROLL = True
LINES = 60 // PARTS
ROWS = 2 * LINES
PITCH = 248
HIGHEST = lax.Precision.HIGHEST
f32 = jnp.float32


def dot(a, b):
    return jnp.dot(a, b, precision=HIGHEST, preferred_element_type=f32)


def half_matrices():
    k, n = np.arange(HALF), np.arange(HALF)
    mats = []
    for odd in range(2):
        angle = 2.0 * math.pi * ((k[:, None] * (2 * n + odd)[None, :]) % N) / N
        cos, sin = np.cos(angle) / math.sqrt(N), np.sin(angle) / math.sqrt(N)
        mats.append(np.stack([np.stack([cos, sin], axis=1), np.stack([-sin, cos], axis=1)]))
    return np.stack(mats)


def x_matrices():
    mat = half_matrices().reshape(2, 2, 2, PARTS, LINES, 2, HALF)
    return mat.transpose(0, 3, 2, 4, 1, 5, 6).reshape(2, N, N).astype(np.float32)


def y_matrices():
    return half_matrices().reshape(2, N, N).astype(np.float32)


def z_matrix(cols):
    k = np.arange(N)
    angle = 2.0 * math.pi * ((k[:, None] * k[None, :]) % N) / N
    cos, sin = np.cos(angle) / math.sqrt(N), np.sin(angle) / math.sqrt(N)
    mat = np.zeros((cols, 2, LANES, 2, 256))
    for b in range(cols):
        part = slice(b * HALF, (b + 1) * HALF)
        mat[b, 0, :HALF, 0, :N], mat[b, 1, :HALF, 0, :N] = cos[part], sin[part]
        mat[b, 0, :HALF, 1, :N], mat[b, 1, :HALF, 1, :N] = -sin[part], cos[part]
    return mat.reshape(cols * 2 * LANES, 512).astype(np.float32)


def lane_index(rows):
    return lax.broadcasted_iota(jnp.int32, (rows, LANES), 1)


def gather_spread(parts):
    lane = lane_index(8)
    out = jnp.zeros((8, LANES), f32)
    for m, part in enumerate(parts):
        moved = pltpu.roll(part, (SPARE * m - HALF) % LANES, 1)
        out = jnp.where((lane >= SPARE * m) & (lane < SPARE * (m + 1)), moved, out)
    return out


def x_body(parts, scalars, ur, ui, er, ei, mat_e, mat_o, *refs):
    own, near, *far = refs[-2 - 2 * parts:]
    lane = lane_index(HALF)
    core, chip = scalars[0] % 2, scalars[0] // 2
    sign = jnp.where(chip == 0, 1.0, -1.0).astype(f32)

    def samples(slot, odd):
        j = pl.program_id(0) * X_BLOCK + slot + scalars[2]
        shift = HALF - SPARE * lax.rem(j, SPREAD)
        extra = jnp.minimum(j // SPREAD, 2)
        rows = pl.ds(odd, HALF, stride=2)
        pieces = []
        for u, e in ((ur, er), (ui, ei)):
            moved = pltpu.roll(e.at[0, extra][rows, :], shift, 1)
            pieces.append(jnp.where(lane < HALF, u.at[0, slot][rows, :], moved))
        return jnp.concatenate(pieces, axis=0)

    def matrix(mat):
        return jnp.concatenate([mat[pl.ds(pl.multiple_of((2 * p + (core ^ d)) * ROWS, 8), ROWS), :] for p in range(parts) for d in range(2)], axis=0)

    for first in range(0, X_BLOCK, 2):
        slots = [first, first + 1]
        even = dot(matrix(mat_e), jnp.concatenate([samples(s, 0) for s in slots], axis=1))
        odd = sign * dot(matrix(mat_o), jnp.concatenate([samples(s, 1) for s in slots], axis=1))
        both = (even + odd, even - odd)
        for i, s in enumerate(slots):
            for p in range(parts):
                for d in range(4):
                    block = both[d // 2][(2 * p + d % 2) * ROWS:(2 * p + d % 2 + 1) * ROWS, i * LANES:(i + 1) * LANES]
                    if d < 2:
                        (own, near)[d][s, p * ROWS:(p + 1) * ROWS] = block
                    else:
                        far[2 * p + d - 2][s] = block


def y_body(scalars, r0, r1, r2, r3, mat_e, mat_o, *refs):
    own, other, lines = refs[-3:]
    sign = jnp.where(scalars[1] == 0, 1.0, -1.0).astype(f32)
    for d, r in enumerate((r0, r1, r2, r3)):
        base = (scalars[0] ^ d) * 30
        groups = [r[j] for j in range(SLOTS)]
        groups += [gather_spread(groups[SPREAD * i:SPREAD * (i + 1)]) for i in range(3)]
        for y, v in enumerate(groups):
            lines[pl.ds(base + (y % 2 * HALF + y // 2), 8, stride=PITCH), :] = v
    lane = lane_index(8)

    def pair(p, carry):
        def samples(odd):
            rows = lambda kx, c: pl.ds(pl.multiple_of((2 * kx + c) * PITCH + odd * HALF, 8), HALF)
            return jnp.concatenate([jnp.concatenate([lines[rows(2 * p + j, c), :] for c in range(2)], axis=0) for j in range(2)], axis=1)

        even = dot(mat_e[...], samples(0))
        odd = sign * dot(mat_o[...], samples(1))
        mine, sent = even + odd, even - odd
        own[2 * p] = mine[:, :LANES]
        own[2 * p + 1] = mine[:, LANES:]
        groups = [sent[8 * (j % 30):8 * (j % 30) + 8, j // 30 * LANES:(j // 30 + 1) * LANES] for j in range(60)]
        for j in range(SLOTS):
            v = groups[j]
            if j < 3 * SPREAD:
                v = jnp.where(lane < HALF, v, pltpu.roll(groups[SLOTS + j // SPREAD], HALF - SPARE * (j % SPREAD), 1))
            other[p, 8 * j:8 * j + 8] = v
        return carry

    if Y_UNROLL:
        for p in range(2):
            pair(p, 0)
    else:
        lax.fori_loop(0, 2, pair, 0)


def z_body(scalars, t, q, g, mat, *refs):
    wr, wi, _ = refs[-3:]
    lane = lane_index(N)
    me = scalars[1]

    def matrix():
        return jnp.concatenate([mat[pl.ds(pl.multiple_of((me ^ d) * 256, 8), 256), :] for d in range(2)], axis=0)

    def pair(p, carry):
        line = refs[-1]
        for j in range(2):
            line[2 * j] = jnp.where(lane < HALF, t[2 * p + j], 0.0)
        line[1] = jnp.where(lane < HALF, q[p, :N], 0.0)
        line[3, :216] = jnp.where(lane[:216] < HALF, q[p, N:], 0.0)
        for i in range(3):
            line[3, 216 + 8 * i:224 + 8 * i] = gather_spread([q[p, 8 * j:8 * j + 8] for j in range(SPREAD * i, SPREAD * (i + 1))])
        lhs = jnp.concatenate([jnp.concatenate([line[2 * j + b, c * HALF:(c + 1) * HALF] for b in range(2) for c in range(2)], axis=1)
                               for j in range(2)], axis=0)
        res = dot(lhs, matrix())
        for j in range(2):
            part = res[j * HALF:(j + 1) * HALF]
            wr[0, 2 * p + j] = part[:, :N] * g[2 * p + j]
            wi[0, 2 * p + j] = part[:, 256:256 + N] * g[2 * p + j]
        return carry

    lax.fori_loop(0, 2, pair, 0)


def solution(mesh):
    rows, cols = mesh.shape["row"], mesh.shape["col"]
    params = pltpu.CompilerParams(vmem_limit_bytes=63 * 2**20)
    cost = pl.CostEstimate(flops=6 * 2 * 480 * 480 * 7200, bytes_accessed=30_000_000, transcendentals=0)
    once = pl.Buffered(1)
    unread = pl.BlockSpec(memory_space=pl.ANY)
    smem = pl.BlockSpec(memory_space=pltpu.SMEM)

    def local_forward(u_real, u_imag, g_filter):
        fields = u_real.shape[0]
        ur, ui = jnp.transpose(u_real, (0, 2, 1, 3)), jnp.transpose(u_imag, (0, 2, 1, 3))
        scalars = jnp.stack([lax.axis_index("row"), lax.axis_index("col"), 0])
        (xe, xo), (ye, yo), mat_z = x_matrices(), y_matrices(), z_matrix(cols)
        last = []

        def call(body, args, specs, **kw):
            out = pl.pallas_call(body, in_specs=[smem] + specs + [unread] * len(last), compiler_params=params, cost_estimate=cost, **kw)(scalars, *args, *last)
            last[:] = [out[0]]
            return out

        def x_step(f, first, parts):
            spec = pl.BlockSpec((1, X_BLOCK, N, LANES), lambda i: (f, i, 0, 0))
            extra = pl.BlockSpec((1, 3, N, LANES), lambda i: (f, SLOTS // 3, 0, 0), pipeline_mode=once)
            used = slice(first * 2 * ROWS, (first + parts) * 2 * ROWS)
            mat = pl.BlockSpec((parts * 2 * ROWS, N), lambda i: (0, 0), pipeline_mode=once)
            sizes = [parts * ROWS] * 2 + [ROWS] * (2 * parts)
            return call(
                lambda *a: x_body(parts, *a), (ur, ui, ur, ui, xe[used], xo[used]), [spec, spec, extra, extra, mat, mat], grid=(60 // X_BLOCK,),
                out_specs=[pl.BlockSpec((X_BLOCK, n, LANES), lambda i: (i, 0, 0)) for n in sizes],
                out_shape=[jax.ShapeDtypeStruct((SLOTS, n, LANES), f32) for n in sizes], name="xstep")

        def y_step(p, own, near, far0, far1):
            mat = pl.BlockSpec((N, N), lambda i: (0, 0), pipeline_mode=once)
            wide = pl.BlockSpec((SLOTS, 8, LANES), lambda i: (0, p * (ROWS // 8) + i, 0))
            part = pl.BlockSpec((SLOTS, 8, LANES), lambda i: (0, i, 0))
            return call(
                y_body, (own, near, far0, far1, ye, yo), [wide, wide, part, part, mat, mat], grid=(LINES // 4,),
                out_specs=[pl.BlockSpec((4, N, LANES), lambda i: (i, 0, 0)), pl.BlockSpec((2, 8 * SLOTS, LANES), lambda i: (i, 0, 0))],
                out_shape=[jax.ShapeDtypeStruct((LINES, N, LANES), f32), jax.ShapeDtypeStruct((LINES // 2, 8 * SLOTS, LANES), f32)],
                scratch_shapes=[pltpu.VMEM((8 * PITCH, LANES), f32)], name="ystep")

        def z_step(f, h, t, q, w):
            lines = lambda i: h * (LINES // 4) + i
            spec = pl.BlockSpec((1, 4, HALF, N), lambda i: (f, lines(i), 0, 0))
            shape = jax.ShapeDtypeStruct((fields, 60, HALF, N), f32)
            if w and last[0] is w[0]:
                last.clear()
            return call(
                z_body, (t, q, g_filter, mat_z, *w),
                [pl.BlockSpec((4, N, LANES), lambda i: (i, 0, 0)), pl.BlockSpec((2, 8 * SLOTS, LANES), lambda i: (i, 0, 0)),
                 pl.BlockSpec((4, HALF, N), lambda i: (lines(i), 0, 0)), pl.BlockSpec((512, 512), lambda i: (0, 0), pipeline_mode=once)]
                + [unread] * len(w),
                grid=(LINES // 4,), out_specs=[spec, spec], out_shape=[shape, shape], input_output_aliases={5: 0, 6: 1} if w else {},
                scratch_shapes=[pltpu.VMEM((4, N, LANES), f32)], name="zstep")

        def swap(v, axis, d, size):
            return lax.ppermute(v, axis, [(i, i ^ d) for i in range(size)])

        arrived = {}

        def send_x(f, first, parts):
            own, near, *far = x_step(f, first, parts)
            near = swap(near, "row", 1, rows)
            for p in range(parts):
                arrived[f * PARTS + first + p] = (p, own, near, swap(far[2 * p], "row", 2, rows), swap(far[2 * p + 1], "row", 3, rows))

        send_x(0, 0, 1)
        send_x(0, 1, PARTS - 1)
        w, waiting = (), None
        for k in range(fields * PARTS):
            t, sent = y_step(*arrived.pop(k))
            q = swap(sent, "col", 1, cols)
            if k % PARTS == 0 and k // PARTS + 1 < fields:
                send_x(k // PARTS + 1, 0, PARTS)
            if waiting:
                w = z_step(*waiting, w)
            waiting = (k // PARTS, k % PARTS, t, q)
        w = z_step(*waiting, w)
        return w[0], w[1]

    field_spec = P("fld", None, "row", "col")
    out_spec = P("fld", "row", "col", None)
    return jax.shard_map(local_forward, mesh=mesh, in_specs=(field_spec, field_spec, P("row", "col", None)), out_specs=(out_spec, out_spec), check_vma=False)
```

```python
import math
import numpy as np
import jax
import jax.numpy as jnp
from jax import lax
from jax.experimental import pallas as pl
from jax.experimental.pallas import tpu as pltpu
from jax.sharding import PartitionSpec as P


N = 240
HALF = N // 2
LANES = 128
SLOTS = 57
SPARE = LANES - HALF
SPREAD = HALF // SPARE
PARTS = 5
X_BLOCK = 4
X_WIDE = 4
LINES = 60 // PARTS
ROWS = 2 * LINES
PITCH = 248
HIGHEST = lax.Precision.HIGHEST
f32 = jnp.float32


def dot(a, b):
    return jnp.dot(a, b, precision=HIGHEST, preferred_element_type=f32)


def half_matrices():
    k, n = np.arange(HALF), np.arange(HALF)
    mats = []
    for odd in range(2):
        angle = 2.0 * math.pi * ((k[:, None] * (2 * n + odd)[None, :]) % N) / N
        cos, sin = np.cos(angle) / math.sqrt(N), np.sin(angle) / math.sqrt(N)
        mats.append(np.stack([np.stack([cos, sin], axis=1), np.stack([-sin, cos], axis=1)]))
    return np.stack(mats)


def x_matrices():
    mat = half_matrices().reshape(2, 2, 2, PARTS, LINES, 2, HALF)
    return mat.transpose(0, 3, 2, 4, 1, 5, 6).reshape(2, N, N).astype(np.float32)


def y_matrices():
    return half_matrices().reshape(2, N, N).astype(np.float32)


def z_matrix(cols):
    k = np.arange(N)
    angle = 2.0 * math.pi * ((k[:, None] * k[None, :]) % N) / N
    cos, sin = np.cos(angle) / math.sqrt(N), np.sin(angle) / math.sqrt(N)
    mat = np.zeros((cols, 2, LANES, 2, 256))
    for b in range(cols):
        part = slice(b * HALF, (b + 1) * HALF)
        mat[b, 0, :HALF, 0, :N], mat[b, 1, :HALF, 0, :N] = cos[part], sin[part]
        mat[b, 0, :HALF, 1, :N], mat[b, 1, :HALF, 1, :N] = -sin[part], cos[part]
    return mat.reshape(cols * 2 * LANES, 512).astype(np.float32)


def lane_index(rows):
    return lax.broadcasted_iota(jnp.int32, (rows, LANES), 1)


def gather_spread(parts):
    lane = lane_index(8)
    out = jnp.zeros((8, LANES), f32)
    for m, part in enumerate(parts):
        moved = pltpu.roll(part, (SPARE * m - HALF) % LANES, 1)
        out = jnp.where((lane >= SPARE * m) & (lane < SPARE * (m + 1)), moved, out)
    return out


def x_body(parts, scalars, *refs):
    us, (er, ei, mat_e, mat_o) = refs[:2 * X_BLOCK], refs[2 * X_BLOCK:2 * X_BLOCK + 4]
    own, near, *far = refs[-2 - 2 * parts:]
    lane = lane_index(HALF)
    core, chip = scalars[0] % 2, scalars[0] // 2
    sign = jnp.where(chip == 0, 1.0, -1.0).astype(f32)

    def samples(slot, odd):
        j = pl.program_id(0) * X_BLOCK + slot
        shift = HALF - SPARE * lax.rem(j, SPREAD)
        extra = jnp.minimum(j // SPREAD, 2)
        rows = pl.ds(odd, HALF, stride=2)
        pieces = []
        for u, e in ((us[slot], er), (us[X_BLOCK + slot], ei)):
            moved = pltpu.roll(e.at[0, extra][rows, :], shift, 1)
            pieces.append(jnp.where(lane < HALF, u.at[0, 0][rows, :], moved))
        return jnp.concatenate(pieces, axis=0)

    def matrix(mat):
        return jnp.concatenate([mat[pl.ds(pl.multiple_of((2 * p + (core ^ d)) * ROWS, 8), ROWS), :] for p in range(parts) for d in range(2)], axis=0)

    for first in range(0, X_BLOCK, X_WIDE):
        slots = list(range(first, first + X_WIDE))
        even = dot(matrix(mat_e), jnp.concatenate([samples(s, 0) for s in slots], axis=1))
        odd = sign * dot(matrix(mat_o), jnp.concatenate([samples(s, 1) for s in slots], axis=1))
        both = (even + odd, even - odd)
        for i, s in enumerate(slots):
            for p in range(parts):
                for d in range(4):
                    block = both[d // 2][(2 * p + d % 2) * ROWS:(2 * p + d % 2 + 1) * ROWS, i * LANES:(i + 1) * LANES]
                    if d < 2:
                        (own, near)[d][s, p * ROWS:(p + 1) * ROWS] = block
                    else:
                        far[2 * p + d - 2][s] = block


def y_body(first_row, scalars, *refs):
    sources, (mat_e, mat_o) = refs[:4], refs[4:6]
    own, other, inputs, lines, mine_buf, sent_buf, in_sem, out_sem = refs[-8:]
    sign = jnp.where(scalars[1] == 0, 1.0, -1.0).astype(f32)
    lane = lane_index(8)
    groups = LINES // 4

    def fetch(g, d):
        row = pl.multiple_of((first_row if d < 2 else 0) + 8 * g, 8)
        return pltpu.make_async_copy(sources[d].at[:, pl.ds(row, 8), :], inputs.at[g, d], in_sem.at[g, d])

    def put(g):
        return ([pltpu.make_async_copy(mine_buf.at[4 * g + j], own.at[4 * g + j], out_sem.at[g]) for j in range(4)]
                + [pltpu.make_async_copy(sent_buf.at[2 * g + p], other.at[2 * g + p], out_sem.at[g]) for p in range(2)])

    for g in range(groups):
        for d in range(4):
            fetch(g, d).start()

    def group(g, carry):
        for d in range(4):
            fetch(g, d).wait()
            base = (scalars[0] ^ d) * 30
            slots = [inputs[g, d, j] for j in range(SLOTS)]
            slots += [gather_spread(slots[SPREAD * i:SPREAD * (i + 1)]) for i in range(3)]
            for y, v in enumerate(slots):
                lines[pl.ds(base + (y % 2 * HALF + y // 2), 8, stride=PITCH), :] = v
        for p in range(2):
            def samples(odd):
                rows = lambda kx, c: pl.ds((2 * kx + c) * PITCH + odd * HALF, HALF)
                return jnp.concatenate([jnp.concatenate([lines[rows(2 * p + j, c), :] for c in range(2)], axis=0) for j in range(2)], axis=1)

            even = dot(mat_e[...], samples(0))
            odd = sign * dot(mat_o[...], samples(1))
            mine, sent = even + odd, even - odd
            mine_buf[4 * g + 2 * p] = mine[:, :LANES]
            mine_buf[4 * g + 2 * p + 1] = mine[:, LANES:]
            rows = [sent[8 * (j % 30):8 * (j % 30) + 8, j // 30 * LANES:(j // 30 + 1) * LANES] for j in range(60)]
            for j in range(SLOTS):
                v = rows[j]
                if j < 3 * SPREAD:
                    v = jnp.where(lane < HALF, v, pltpu.roll(rows[SLOTS + j // SPREAD], HALF - SPARE * (j % SPREAD), 1))
                sent_buf[2 * g + p, 8 * j:8 * j + 8] = v
        for c in put(g):
            c.start()
        return carry

    lax.fori_loop(0, groups, group, 0)
    for g in range(groups):
        for c in put(g):
            c.wait()


def z_body(field, first, count, scalars, t, q, g_hbm, mat, *refs):
    wr, wi, t_buf, q_buf, g_buf, out_buf, line, t_sem, q_sem, g_sem, out_sem = refs[-11:]
    lane = lane_index(N)
    me = scalars[1]

    def fetch(i):
        return ([pltpu.make_async_copy(t.at[4 * i + j], t_buf.at[4 * i + j], t_sem.at[i]) for j in range(4)]
                + [pltpu.make_async_copy(q.at[2 * i + p], q_buf.at[2 * i + p], q_sem.at[i]) for p in range(2)]
                + [pltpu.make_async_copy(g_hbm.at[first + 4 * i + j], g_buf.at[4 * i + j], g_sem.at[i]) for j in range(4)])

    def put(i):
        return [pltpu.make_async_copy(out_buf.at[c, 4 * i + j], w.at[field, first + 4 * i + j], out_sem.at[i])
                for j in range(4) for c, w in enumerate((wr, wi))]

    for i in range(count // 4):
        for c in fetch(i):
            c.start()

    def group(i, carry):
        for c in fetch(i):
            c.wait()
        for p in range(2):
            for j in range(2):
                line[4 * p + 2 * j] = jnp.where(lane < HALF, t_buf[4 * i + 2 * p + j], 0.0)
            line[4 * p + 1] = jnp.where(lane < HALF, q_buf[2 * i + p, :N], 0.0)
            line[4 * p + 3, :216] = jnp.where(lane[:216] < HALF, q_buf[2 * i + p, N:], 0.0)
            for m in range(3):
                line[4 * p + 3, 216 + 8 * m:224 + 8 * m] = gather_spread([q_buf[2 * i + p, 8 * j:8 * j + 8] for j in range(SPREAD * m, SPREAD * (m + 1))])
        lhs = jnp.concatenate([jnp.concatenate([line[2 * j + b, c * HALF:(c + 1) * HALF] for b in range(2) for c in range(2)], axis=1)
                               for j in range(4)], axis=0)
        order = jnp.concatenate([mat[pl.ds(pl.multiple_of((me ^ d) * 256, 8), 256), :] for d in range(2)], axis=0)
        res = dot(lhs, order)
        for j in range(4):
            part = res[j * HALF:(j + 1) * HALF]
            for c in range(2):
                out_buf[c, 4 * i + j] = part[:, 256 * c:256 * c + N] * g_buf[4 * i + j]
        for c in put(i):
            c.start()
        return carry

    lax.fori_loop(0, count // 4, group, 0)
    for i in range(count // 4):
        for c in put(i):
            c.wait()


def solution(mesh):
    rows, cols = mesh.shape["row"], mesh.shape["col"]
    params = pltpu.CompilerParams(vmem_limit_bytes=63 * 2**20)
    cost = pl.CostEstimate(flops=6 * 2 * 480 * 480 * 7200, bytes_accessed=30_000_000, transcendentals=0)
    once = pl.Buffered(1)
    unread = pl.BlockSpec(memory_space=pl.ANY)
    smem = pl.BlockSpec(memory_space=pltpu.SMEM)

    def local_forward(u_real, u_imag, g_filter):
        fields = u_real.shape[0]
        ur, ui = jnp.transpose(u_real, (0, 2, 1, 3)), jnp.transpose(u_imag, (0, 2, 1, 3))
        scalars = jnp.stack([lax.axis_index("row"), lax.axis_index("col")])
        (xe, xo), (ye, yo), mat_z = x_matrices(), y_matrices(), z_matrix(cols)
        last = []

        def call(body, args, specs, **kw):
            out = pl.pallas_call(body, in_specs=[smem] + specs + [unread] * len(last), compiler_params=params, cost_estimate=cost, **kw)(scalars, *args, *last)
            last[:] = [out[0]]
            return out

        def x_step(f, first, parts):
            one = [pl.BlockSpec((1, 1, N, LANES), lambda i, s=s: (f, X_BLOCK * i + s, 0, 0)) for s in range(X_BLOCK)]
            extra = pl.BlockSpec((1, 3, N, LANES), lambda i: (f, SLOTS // 3, 0, 0), pipeline_mode=once)
            used = slice(first * 2 * ROWS, (first + parts) * 2 * ROWS)
            mat = pl.BlockSpec((parts * 2 * ROWS, N), lambda i: (0, 0), pipeline_mode=once)
            sizes = [parts * ROWS] * 2 + [ROWS] * (2 * parts)
            return call(
                lambda *a: x_body(parts, *a), [ur] * X_BLOCK + [ui] * X_BLOCK + [ur, ui, xe[used], xo[used]], one + one + [extra, extra, mat, mat],
                grid=(60 // X_BLOCK,), out_specs=[pl.BlockSpec((X_BLOCK, n, LANES), lambda i: (i, 0, 0)) for n in sizes],
                out_shape=[jax.ShapeDtypeStruct((SLOTS, n, LANES), f32) for n in sizes], name="xstep")

        whole = pl.BlockSpec(memory_space=pltpu.VMEM)
        vmem = lambda *shape: pltpu.VMEM(shape, f32)
        sems = lambda *shape: pltpu.SemaphoreType.DMA(shape)

        def y_step(p, own, near, far0, far1):
            return call(
                lambda *a: y_body(p * ROWS, *a), (own, near, far0, far1, ye, yo), [unread] * 4 + [whole, whole], out_specs=[unread] * 2,
                out_shape=[jax.ShapeDtypeStruct((LINES, N, LANES), f32), jax.ShapeDtypeStruct((LINES // 2, 8 * SLOTS, LANES), f32)],
                scratch_shapes=[vmem(LINES // 4, 4, SLOTS, 8, LANES), vmem(8 * PITCH, LANES), vmem(LINES, N, LANES), vmem(LINES // 2, 8 * SLOTS, LANES),
                                sems(LINES // 4, 4), sems(LINES // 4)], name="ystep")

        def z_step(f, h, t, q, w):
            shape = jax.ShapeDtypeStruct((fields, 60, HALF, N), f32)
            if w and last[0] is w[0]:
                last.clear()
            return call(
                lambda *a: z_body(f, h * LINES, LINES, *a), (t, q, g_filter, mat_z, *w), [unread] * 3 + [whole] + [unread] * len(w),
                out_specs=[unread] * 2, out_shape=[shape, shape], input_output_aliases={5: 0, 6: 1} if w else {},
                scratch_shapes=[vmem(LINES, N, LANES), vmem(LINES // 2, 8 * SLOTS, LANES), vmem(LINES, HALF, N), vmem(2, LINES, HALF, N), vmem(8, N, LANES)]
                + [sems(LINES // 4)] * 4, name="zstep")

        def swap(v, axis, d, size):
            return lax.ppermute(v, axis, [(i, i ^ d) for i in range(size)])

        arrived = {}

        def send_x(f, first, parts):
            own, near, *far = x_step(f, first, parts)
            near = swap(near, "row", 1, rows)
            for p in range(parts):
                arrived[f * PARTS + first + p] = (p, own, near, swap(far[2 * p], "row", 2, rows), swap(far[2 * p + 1], "row", 3, rows))

        send_x(0, 0, 1)
        send_x(0, 1, PARTS - 1)
        w, waiting = (), []
        for k in range(fields * PARTS):
            t, sent = y_step(*arrived.pop(k))
            q = swap(sent, "col", 1, cols)
            if k % PARTS == 0 and k // PARTS + 1 < fields:
                send_x(k // PARTS + 1, 0, PARTS)
            else:
                while waiting:
                    w = z_step(*waiting.pop(0), w)
            waiting.append((k // PARTS, k % PARTS, t, q))
        for item in waiting:
            w = z_step(*item, w)
        return w[0], w[1]

    field_spec = P("fld", None, "row", "col")
    out_spec = P("fld", "row", "col", None)
    return jax.shard_map(local_forward, mesh=mesh, in_specs=(field_spec, field_spec, P("row", "col", None)), out_specs=(out_spec, out_spec), check_vma=False)
```

```python
import math
import numpy as np
import jax
import jax.numpy as jnp
from jax import lax
from jax.experimental import pallas as pl
from jax.experimental.pallas import tpu as pltpu
from jax.sharding import PartitionSpec as P


N = 240
HALF = N // 2
LANES = 128
PARTS = 5
LINES = 60 // PARTS
ROWS = 2 * LINES
PITCH = 248
SPARE = LANES - HALF
SPREAD = HALF // SPARE
MAIN = 56
LEFT = MAIN - 3 * SPREAD
X_ROWS = MAIN * ROWS + 8
X_BLOCK = 12
KEPT = 113
HIGHEST = lax.Precision.HIGHEST
f32 = jnp.float32


def dot(a, b):
    return jnp.dot(a, b, precision=HIGHEST, preferred_element_type=f32)


def half_matrices():
    k, n = np.arange(HALF), np.arange(HALF)
    mats = []
    for odd in range(2):
        angle = 2.0 * math.pi * ((k[:, None] * (2 * n + odd)[None, :]) % N) / N
        cos, sin = np.cos(angle) / math.sqrt(N), np.sin(angle) / math.sqrt(N)
        mats.append(np.stack([np.stack([cos, sin], axis=1), np.stack([-sin, cos], axis=1)]))
    return np.stack(mats)


def x_matrices():
    mat = half_matrices().reshape(2, 2, 2, PARTS, LINES, 2, HALF)
    return mat.transpose(0, 3, 2, 4, 1, 5, 6).reshape(2, N, N).astype(np.float32)


def y_matrices():
    return half_matrices().reshape(2, N, N).astype(np.float32)


def z_matrix(cols):
    k = np.arange(N)
    angle = 2.0 * math.pi * ((k[:, None] * k[None, :]) % N) / N
    cos, sin = np.cos(angle) / math.sqrt(N), np.sin(angle) / math.sqrt(N)
    mat = np.zeros((cols, 2, LANES, 2, 256))
    for b in range(cols):
        part = slice(b * HALF, (b + 1) * HALF)
        mat[b, 0, :HALF, 0, :N], mat[b, 1, :HALF, 0, :N] = cos[part], sin[part]
        mat[b, 0, :HALF, 1, :N], mat[b, 1, :HALF, 1, :N] = -sin[part], cos[part]
    return mat.reshape(cols * 2 * LANES, 512).astype(np.float32)


def lane_index(rows):
    return lax.broadcasted_iota(jnp.int32, (rows, LANES), 1)


def gather_spread(parts):
    lane = lane_index(8)
    out = jnp.zeros((8, LANES), f32)
    for m, part in enumerate(parts):
        moved = pltpu.roll(part, (SPARE * m - HALF) % LANES, 1)
        out = jnp.where((lane >= SPARE * m) & (lane < SPARE * (m + 1)), moved, out)
    return out


def x_body(parts, start, scalars, ur, ui, er, ei, mat_e, mat_o, *refs):
    own, near, *far = refs[-2 - 2 * parts:]
    lane = lane_index(HALF)
    core, chip = scalars[0] % 2, scalars[0] // 2
    sign = jnp.where(chip == 0, 1.0, -1.0).astype(f32)
    step = pl.program_id(0) + start

    def out(p, d):
        return (own, near)[d].at[p] if d < 2 else far[2 * p + d - 2]

    def samples(slot, odd):
        j = step * X_BLOCK + slot
        extra = j // SPREAD
        shift = HALF - SPARE * (j - SPREAD * extra)
        rows = pl.ds(odd, HALF, stride=2)
        pieces = []
        for u, e in ((ur, er), (ui, ei)):
            moved = pltpu.roll(e.at[0, extra][rows, :], shift, 1)
            pieces.append(jnp.where(lane < HALF, u.at[0, slot][rows, :], moved))
        return jnp.concatenate(pieces, axis=0)

    def matrix(mat):
        return jnp.concatenate([mat[pl.ds(pl.multiple_of((2 * p + (core ^ d)) * ROWS, 8), ROWS), :] for p in range(parts) for d in range(2)], axis=0)

    def four(b, carry):
        slots = [4 * b + s for s in range(4)]
        even = dot(matrix(mat_e), jnp.concatenate([samples(s, 0) for s in slots], axis=1))
        odd = sign * dot(matrix(mat_o), jnp.concatenate([samples(s, 1) for s in slots], axis=1))
        both = (even + odd, even - odd)

        def block(p, d, i):
            return both[d // 2][(2 * p + d % 2) * ROWS:(2 * p + d % 2 + 1) * ROWS, i * LANES:(i + 1) * LANES]

        for i, s in enumerate(slots):
            for p in range(parts):
                for d in range(4):
                    out(p, d)[pl.ds(pl.multiple_of(s * ROWS, 8), ROWS), :] = block(p, d, i)

        @pl.when(step * X_BLOCK + 4 * b == N // 4 - 4)
        def _():
            lane8 = lane_index(8)
            for p in range(parts):
                for d in range(4):
                    rest = jnp.zeros((8, LANES), f32)
                    for r in range(ROWS // 8):
                        moved = pltpu.roll(block(p, d, 3)[8 * r:8 * r + 8], (32 * r - SPARE * LEFT) % LANES, 1)
                        rest = jnp.where((lane8 >= 32 * r) & (lane8 < 32 * r + 32), moved, rest)
                    out(p, d)[pl.ds((MAIN % X_BLOCK) * ROWS, 8), :] = rest

        return carry

    lax.fori_loop(0, X_BLOCK // 4, four, 0)


def y_body(p, cuts, scalars, *refs):
    own_in, near_in, far0, far1, mat_e, mat_o = refs[:6]
    own, *others = refs[-11 - len(cuts):-10]
    inputs, lines, sent_raw, mine_buf, sent_buf, buf_e, buf_o, in_sem, mat_sem, out_sem = refs[-10:]
    sources = (own_in.at[p], near_in.at[p], far0, far1)
    sign = jnp.where(scalars[1] == 0, 1.0, -1.0).astype(f32)
    lane = lane_index(8)
    groups = LINES // 4
    half = X_ROWS // 16 * 8
    halves = (pl.ds(0, half), pl.ds(half, X_ROWS - half))

    def fetch(d):
        return [pltpu.make_async_copy(sources[d].at[h], inputs.at[d, h], in_sem.at[d]) for h in halves]

    mats = [pltpu.make_async_copy(mat_e, buf_e, mat_sem), pltpu.make_async_copy(mat_o, buf_o, mat_sem)]

    def put(g):
        where = [(o, i) for o, size in zip(others, cuts) for i in range(size)][g]
        return ([pltpu.make_async_copy(mine_buf.at[4 * g + j], own.at[4 * g + j], out_sem.at[g]) for j in range(4)]
                + [pltpu.make_async_copy(sent_buf.at[g], where[0].at[where[1]], out_sem.at[g])])

    for d in range(4):
        for c in fetch(d):
            c.start()
    for c in mats:
        c.start()
    for d in range(4):
        for c in fetch(d):
            c.wait()
    for c in mats:
        c.wait()

    def group(g, carry):
        for d in range(4):
            base = (scalars[0] ^ d) * 30
            slots = [inputs[d, pl.ds(pl.multiple_of(j * ROWS + 8 * g, 8), 8), :] for j in range(MAIN)]
            spread = [gather_spread(slots[SPREAD * i:SPREAD * (i + 1)]) for i in range(4)]
            moved = pltpu.roll(inputs[d, pl.ds(MAIN * ROWS, 8), :], lax.rem(SPARE * LEFT - 32 * g + LANES, LANES), 1)
            spread[3] = jnp.where((lane >= SPARE * LEFT) & (lane < HALF), moved, spread[3])
            for y, v in enumerate(slots + spread):
                lines[pl.ds(base + (y % 2 * HALF + y // 2), 8, stride=PITCH), :] = v
        for q in range(2):
            def samples(odd):
                rows = lambda kx, c: pl.ds((2 * kx + c) * PITCH + odd * HALF, HALF)
                return jnp.concatenate([jnp.concatenate([lines[rows(2 * q + j, c), :] for c in range(2)], axis=0) for j in range(2)], axis=1)

            even = dot(buf_e[...], samples(0))
            odd = sign * dot(buf_o[...], samples(1))
            mine, sent = even + odd, even - odd
            for j in range(2):
                mine_buf[4 * g + 2 * q + j] = mine[:, j * LANES:(j + 1) * LANES]
                sent_raw[(2 * q + j) * N:(2 * q + j + 1) * N] = sent[:, j * LANES:(j + 1) * LANES]
        carried = [sent_raw[8 * j:8 * j + 8] for j in range(KEPT, 120)]
        for j in range(KEPT):
            v = sent_raw[8 * j:8 * j + 8]
            if j < len(carried) * SPREAD:
                v = jnp.where(lane < HALF, v, pltpu.roll(carried[j // SPREAD], HALF - SPARE * (j % SPREAD), 1))
            sent_buf[g, 8 * j:8 * j + 8] = v
        return carry

    if len(cuts) == 1:
        def both(g, carry):
            group(g, carry)
            for j in range(4):
                pltpu.make_async_copy(mine_buf.at[4 * g + j], own.at[4 * g + j], out_sem.at[g]).start()
            pltpu.make_async_copy(sent_buf.at[g], others[0].at[g], out_sem.at[g]).start()
            return carry

        lax.fori_loop(0, groups, both, 0)
    else:
        def first(g, carry):
            return group(g, carry)

        lax.fori_loop(0, groups, first, 0)
        for g in range(groups):
            for c in put(g):
                c.start()
    for g in range(groups):
        for c in put(g):
            c.wait()


def z_body(field, first, count, offset, scalars, t, q, g_hbm, mat, *refs):
    wr, wi, t_buf, q_buf, g_buf, out_buf, line, mat_buf, t_sem, q_sem, g_sem, mat_sem, out_sem = refs[-13:]
    lane = lane_index(N)
    me = scalars[1]

    def fetch(i):
        return ([pltpu.make_async_copy(t.at[offset + 4 * i + j], t_buf.at[4 * i + j], t_sem.at[i]) for j in range(4)]
                + [pltpu.make_async_copy(q.at[i], q_buf.at[i], q_sem.at[i])]
                + [pltpu.make_async_copy(g_hbm.at[first + 4 * i + j], g_buf.at[4 * i + j], g_sem.at[i]) for j in range(4)])

    def put(i):
        return [pltpu.make_async_copy(out_buf.at[c, 4 * i + j], w.at[field, first + 4 * i + j], out_sem.at[i])
                for j in range(4) for c, w in enumerate((wr, wi))]

    mats = [pltpu.make_async_copy(mat.at[pl.ds(pl.multiple_of((me ^ d) * 256, 256), 256)], mat_buf.at[pl.ds(256 * d, 256)], mat_sem) for d in range(2)]
    for c in fetch(0) + mats:
        c.start()
    for i in range(1, count // 4):
        for c in fetch(i):
            c.start()
    for c in mats:
        c.wait()

    def group(i, carry):
        for c in fetch(i):
            c.wait()
        for j in range(4):
            line[2 * j] = jnp.where(lane < HALF, t_buf[4 * i + j], 0.0)
            whole = min(N, 8 * KEPT - j * N)
            line[2 * j + 1, :whole] = jnp.where(lane[:whole] < HALF, q_buf[i, j * N:j * N + whole], 0.0)
        for m in range(120 - KEPT):
            row = 8 * (KEPT + m) - 3 * N
            line[7, row:row + 8] = gather_spread([q_buf[i, 8 * j:8 * j + 8] for j in range(SPREAD * m, SPREAD * (m + 1))])
        lhs = jnp.concatenate([jnp.concatenate([line[2 * j + b, c * HALF:(c + 1) * HALF] for b in range(2) for c in range(2)], axis=1)
                               for j in range(4)], axis=0)
        res = dot(lhs, mat_buf[...])
        for j in range(4):
            part = res[j * HALF:(j + 1) * HALF]
            for c in range(2):
                out_buf[c, 4 * i + j] = part[:, 256 * c:256 * c + N] * g_buf[4 * i + j]
        for c in put(i):
            c.start()
        return carry

    lax.fori_loop(0, count // 4, group, 0)
    for i in range(count // 4):
        for c in put(i):
            c.wait()


def solution(mesh):
    rows, cols = mesh.shape["row"], mesh.shape["col"]
    params = pltpu.CompilerParams(vmem_limit_bytes=63 * 2**20)
    cost = pl.CostEstimate(flops=6 * 2 * 480 * 480 * 7200, bytes_accessed=30_000_000, transcendentals=0)
    once = pl.Buffered(1)
    unread = pl.BlockSpec(memory_space=pl.ANY)
    smem = pl.BlockSpec(memory_space=pltpu.SMEM)

    def local_forward(u_real, u_imag, g_filter):
        fields = u_real.shape[0]
        ur, ui = jnp.transpose(u_real, (0, 2, 1, 3)), jnp.transpose(u_imag, (0, 2, 1, 3))
        scalars = jnp.stack([lax.axis_index("row"), lax.axis_index("col")])
        (xe, xo), (ye, yo), mat_z = x_matrices(), y_matrices(), z_matrix(cols)
        last = []

        def call(body, args, specs, **kw):
            out = pl.pallas_call(body, in_specs=[smem] + specs + [unread] * len(last), compiler_params=params, cost_estimate=cost, **kw)(scalars, *args, *last)
            last[:] = [out[0]]
            return out

        vmem = lambda *shape: pltpu.VMEM(shape, f32)
        sems = lambda *shape: pltpu.SemaphoreType.DMA(shape)
        shaped = lambda *shape: jax.ShapeDtypeStruct(shape, f32)

        def x_step(f, first, parts, start, stop, begun=()):
            block = pl.BlockSpec((1, X_BLOCK, N, LANES), lambda i: (f, start + i, 0, 0))
            extra = pl.BlockSpec((1, 4, N, LANES), lambda i: (f, MAIN // 4, 0, 0), pipeline_mode=once)
            used = slice(first * 2 * ROWS, (first + parts) * 2 * ROWS)
            mat = pl.BlockSpec((parts * 2 * ROWS, N), lambda i: (0, 0), pipeline_mode=once)
            return call(
                lambda *a: x_body(parts, start, *a), (ur, ui, ur, ui, xe[used], xo[used], *begun), [block, block, extra, extra, mat, mat] + [unread] * len(begun),
                grid=(stop - start,), input_output_aliases={7 + i: i for i in range(len(begun))},
                out_specs=[pl.BlockSpec((parts, X_BLOCK * ROWS, LANES), lambda i: (0, start + i, 0))] * 2
                + [pl.BlockSpec((X_BLOCK * ROWS, LANES), lambda i: (start + i, 0))] * (2 * parts),
                out_shape=[shaped(parts, X_ROWS, LANES)] * 2 + [shaped(X_ROWS, LANES)] * (2 * parts), name="xstep")

        def y_step(p, own, near, far0, far1, cuts):
            groups = LINES // 4
            return call(
                lambda *a: y_body(p, cuts, *a), (own, near, far0, far1, ye, yo), [unread] * 6, out_specs=[unread] * (1 + len(cuts)),
                out_shape=[shaped(LINES, N, LANES)] + [shaped(c, 8 * KEPT, LANES) for c in cuts],
                scratch_shapes=[vmem(4, X_ROWS, LANES), vmem(8 * PITCH, LANES), vmem(4 * N, LANES), vmem(LINES, N, LANES), vmem(groups, 8 * KEPT, LANES),
                                vmem(N, N), vmem(N, N), sems(4), pltpu.SemaphoreType.DMA, sems(groups)], name="ystep")

        def z_step(f, first, count, offset, t, q, w):
            if w and last[0] is w[0]:
                last.clear()
            return call(
                lambda *a: z_body(f, first, count, offset, *a), (t, q, g_filter, mat_z, *w), [unread] * (4 + len(w)),
                out_specs=[unread] * 2, out_shape=[shaped(fields, 60, HALF, N)] * 2, input_output_aliases={5: 0, 6: 1} if w else {},
                scratch_shapes=[vmem(count, N, LANES), vmem(count // 4, 8 * KEPT, LANES), vmem(count, HALF, N), vmem(2, count, HALF, N), vmem(8, N, LANES),
                                vmem(512, 512), sems(count // 4), sems(count // 4), sems(count // 4), pltpu.SemaphoreType.DMA, sems(count // 4)], name="zstep")

        def swap(v, axis, d, size):
            return lax.ppermute(v, axis, [(i, i ^ d) for i in range(size)])

        arrived = {}

        def send_x(f, first, parts, outs):
            own, near, *far = outs
            near = swap(near, "row", 1, rows)
            for p in range(parts):
                arrived[f * PARTS + first + p] = (p, own, near, swap(far[2 * p], "row", 2, rows), swap(far[2 * p + 1], "row", 3, rows))

        blocks = 60 // X_BLOCK
        send_x(0, 0, 1, x_step(0, 0, 1, 0, blocks))
        send_x(0, 1, PARTS - 1, x_step(0, 1, PARTS - 1, 0, blocks))
        w, waiting, begun, chunks = (), [], (), fields * PARTS
        for k in range(chunks):
            f, h = k // PARTS, k % PARTS
            cuts = (LINES // 4,) if k < chunks - 1 else (LINES // 4 - 1, 1)
            t, *sent = y_step(*arrived.pop(k), cuts)
            sent = [swap(v, "col", 1, cols) for v in sent]
            if h != 1 or f + 1 == fields:
                for item in waiting:
                    w = z_step(*item, w)
                waiting = []
            if f + 1 < fields and h == 0:
                begun = x_step(f + 1, 0, PARTS, 0, 2)
            elif f + 1 < fields and h == 1:
                send_x(f + 1, 0, PARTS, x_step(f + 1, 0, PARTS, 2, blocks, begun))
            done = 0
            for c, q in zip(cuts, sent):
                waiting.append((f, h * LINES + done, 4 * c, done, t, q))
                done += 4 * c
        for item in waiting:
            w = z_step(*item, w)
        return w[0], w[1]

    field_spec = P("fld", None, "row", "col")
    out_spec = P("fld", "row", "col", None)
    return jax.shard_map(local_forward, mesh=mesh, in_specs=(field_spec, field_spec, P("row", "col", None)), out_specs=(out_spec, out_spec), check_vma=False)
```
